32 devices in a mesh: row: 4 (over y, core), col: 4 (over z), depth: 2 (over x).
Axes of the slice: x: 2, y: 2, z: 4, core: 2. Of those that a mesh axis runs over, the one named last changes fastest.
Arguments:
- diag_block: float32 [512, 512], P(('row', 'col', 'depth')), as said below
- panel_rows: float32 [32256, 512], P(('row', 'col', 'depth')), may hold values from -2 to 2
- trailing: float32 [32256, 1024], P(('row', 'depth'), 'col'), may hold values from -6 to 6
Outputs:
- diag_factor: float32 [512, 512], P(('row', 'col', 'depth'))
- panel_factor: float32 [32256, 512], P(('row', 'col', 'depth'))
- updated: float32 [32256, 1024], P(('row', 'depth'), 'col')
The draws below stay inside these ranges and needn't reach their ends.
Inputs may be any that keep to these rules, and one draw needn't show every extreme that they name: `diag_block`: symmetric positive definite.
All inputs are finite; a program needn't handle non-finite values.
Results may differ from the reference program's by a relative error of at most 0.000062.
Values sent between devices are 32-bit elements; how exact they have to be, the bound alone decides.
A program may use at most 64 MiB of HBM per device.

```python
import math
import jax
import jax.numpy as jnp
from jax import lax

PANEL = 512
WIN = 1024
TRAIL = 32256


def draw_diag_block(key, part):
    first = jax.random.fold_in(key, 11)
    second = jax.random.fold_in(key, 12)
    noise = jax.random.normal(first, (PANEL, PANEL), jnp.float32)
    sym = (noise + noise.T) / math.sqrt(2.0 * PANEL)
    shift = jax.random.uniform(second, (PANEL,), jnp.float32, 3.0, 6.0)
    matrix = sym + jnp.diag(shift)
    return matrix


def block_scale(own_key, dims, shards, low, high):
    factor_of = 1.0
    for position, shards_of in shards:
        draws = jax.random.uniform(jax.random.fold_in(jax.random.fold_in(own_key, 6), position), (shards_of,), jnp.float32, low / len(shards), high / len(shards))
        factor_of = factor_of * jnp.repeat(jnp.exp(draws), dims[position] // shards_of).reshape((-1,) + (1,) * (len(dims) - 1 - position))
    return factor_of


def scatter_about(own_key, extent, scale, reach, shards=(), kind=jnp.bfloat16):
    gain = block_scale(own_key, extent, shards, -0.22, 0.18) if shards else 1.0
    result = jax.random.normal(own_key, extent, jnp.float32) * scale * gain
    return jnp.minimum(jnp.maximum(result, -reach), reach).astype(kind)


def setup_inputs(seed: int = 0) -> dict:
    seeds = jax.random.split(jax.random.key(seed), 4)
    diag_block = draw_diag_block(jax.random.fold_in(seeds[3], 71), 0)
    panel_rows = scatter_about(seeds[1], (TRAIL, PANEL), 0.25, 2.0, ((0, 32),), jnp.float32)
    trailing = scatter_about(seeds[2], (TRAIL, WIN), 1.0, 6.0, ((0, 8), (1, 4)), jnp.float32)
    return {"diag_block": diag_block, "panel_rows": panel_rows, "trailing": trailing}


def reference(diag_block, panel_rows, trailing):
    diag_factor = jnp.linalg.cholesky(diag_block)
    panel_factor = jax.scipy.linalg.solve_triangular(diag_factor, panel_rows.T, lower=True).T
    window = panel_factor[:trailing.shape[1]]
    product = lax.dot_general(panel_factor.astype(jnp.float32), window.astype(jnp.float32), (((1,), (1,)), ((), ())), precision=lax.Precision.HIGHEST, preferred_element_type=jnp.float32)
    return (diag_factor, panel_factor, trailing - product)
```

```python
import functools
import math

import jax
import jax.numpy as jnp
from jax import lax
from jax.experimental import pallas as pl
from jax.experimental.pallas import tpu as pltpu
from jax.sharding import PartitionSpec as P

highest = lax.Precision.HIGHEST
AXES = ("row", "col", "depth")
LANES = 128


def dot(left, right, left_dim, right_dim):
    return lax.dot_general(
        left, right, (((left_dim,), (right_dim,)), ((), ())), precision=highest, preferred_element_type=jnp.float32
    )


def factor_block(block):
    size = block.shape[0]
    lane = lax.broadcasted_iota(jnp.int32, (8, size), 1)
    sub = lax.broadcasted_iota(jnp.int32, (8, size), 0)
    tiles = [block[8 * i : 8 * i + 8, :] for i in range(size // 8)]
    for j in range(size):
        t, s = divmod(j, 8)
        row = tiles[t][s : s + 1, :]
        inverse = 1.0 / row[:, j : j + 1]
        source = jnp.where(lane[0:1] == j, 1.0, row) * inverse
        for i in range(t, size // 8):
            if i == t and s == 7:
                continue
            tile = tiles[i]
            new = jnp.where(lane == j, 0.0, tile) - tile[:, j : j + 1] * source
            tiles[i] = jnp.where(sub > s, new, tile) if i == t else new
    whole = jnp.concatenate(tiles, axis=0)
    r_id = lax.broadcasted_iota(jnp.int32, (size, size), 0)
    c_id = lax.broadcasted_iota(jnp.int32, (size, size), 1)
    pivots = jnp.sum(jnp.where(r_id == c_id, whole, 0.0), axis=1, keepdims=True)
    root = jnp.sqrt(pivots)
    scaled = jnp.where(r_id == c_id, 1.0, whole) / root
    inverse = jnp.where(r_id >= c_id, scaled, 0.0)
    upper = jnp.where(r_id < c_id, scaled, jnp.where(r_id == c_id, root, 0.0))
    return upper.T, inverse


def factor_all(work, low, inv, between=None):
    n = work.shape[0]
    low[...] = jnp.zeros((n, n), jnp.float32)
    inv[...] = jnp.zeros((n, n), jnp.float32)

    def step(k, carry):
        at = pl.ds(pl.multiple_of(k * LANES, LANES), LANES)
        block_low, block_inv = factor_block(work[at, at])
        rows = lax.broadcasted_iota(jnp.int32, (n, LANES), 0)
        panel = jnp.where(rows >= (k + 1) * LANES, dot(work[:, at], block_inv, 1, 1), 0.0)
        work[...] = work[...] - dot(panel, panel, 1, 1)
        left = dot(low[at, :], inv[...], 1, 0)
        low[:, at] = panel
        low[at, at] = block_low
        inv[at, :] = -dot(block_inv, left, 1, 0)
        inv[at, at] = block_inv
        if between is not None:
            between(k)
        return carry

    lax.fori_loop(0, n // LANES, step, 0)


def local_factor(diag_ref, low, inv, work):
    work[...] = diag_ref[...]
    factor_all(work, low, inv)


def factor_call(whole_diag):
    shape = jax.ShapeDtypeStruct(whole_diag.shape, jnp.float32)
    n = whole_diag.shape[0]
    return pl.pallas_call(
        local_factor,
        out_shape=(shape, shape),
        scratch_shapes=[pltpu.VMEM((n, n), jnp.float32)],
        cost_estimate=pl.CostEstimate(flops=400_000 * n, bytes_accessed=12 * n * n, transcendentals=0),
    )(whole_diag)


def spread(value, axis, source):
    kept = jnp.where(lax.axis_index(axis) == source, value, 0).astype(value.dtype)
    return lax.psum(kept, axis)


def body(diag_block, panel_rows, trailing):
    position = (
        lax.axis_index("row") * lax.axis_size("col") + lax.axis_index("col")
    ) * lax.axis_size("depth") + lax.axis_index("depth")
    mine = diag_block.shape[0]
    own_rows, win_rows = trailing.shape
    whole_diag = lax.all_gather(diag_block, AXES, axis=0, tiled=True)
    block_row = lax.all_gather(panel_rows, ("col", "depth"), axis=0, tiled=True)
    owned = lax.dynamic_slice_in_dim(block_row, lax.axis_index("depth") * own_rows, own_rows, 0)
    local_window = lax.dynamic_slice_in_dim(block_row, lax.axis_index("col") * win_rows, win_rows, 0)
    full_window = spread(local_window, "row", 0)
    low, inv = factor_call(whole_diag)
    own_factor = lax.dynamic_slice_in_dim(low, position * mine, mine, 0)
    solved = dot(panel_rows, inv, 1, 1)
    weight = dot(dot(full_window, inv, 1, 1), inv, 1, 0)
    updated = trailing - dot(owned, weight, 1, 1)
    return (own_factor, solved, updated)


def solution(mesh):
    specs = (P(AXES, None), P(AXES, None), P(("row", "depth"), "col"))
    return jax.shard_map(body, mesh=mesh, in_specs=specs, out_specs=specs, check_vma=False)
```

```python
import functools
import math

import jax
import jax.numpy as jnp
from jax import lax
from jax.experimental import pallas as pl
from jax.experimental.pallas import tpu as pltpu
from jax.sharding import PartitionSpec as P

highest = lax.Precision.HIGHEST
AXES = ("row", "col", "depth")
LANES = 128


def dot(left, right, left_dim, right_dim):
    return lax.dot_general(
        left, right, (((left_dim,), (right_dim,)), ((), ())), precision=highest, preferred_element_type=jnp.float32
    )


def factor_block(block, halfway=None):
    size = block.shape[0]
    lane = lax.broadcasted_iota(jnp.int32, (8, size), 1)
    sub = lax.broadcasted_iota(jnp.int32, (8, size), 0)
    tiles = [block[8 * i : 8 * i + 8, :] for i in range(size // 8)]
    for j in range(size):
        if halfway is not None and j == size // 2:
            halfway()
        t, s = divmod(j, 8)
        row = tiles[t][s : s + 1, :]
        inverse = 1.0 / row[:, j : j + 1]
        source = jnp.where(lane[0:1] == j, 1.0, row) * inverse
        for i in range(t, size // 8):
            if i == t and s == 7:
                continue
            tile = tiles[i]
            new = jnp.where(lane == j, 0.0, tile) - tile[:, j : j + 1] * source
            tiles[i] = jnp.where(sub > s, new, tile) if i == t else new
    whole = jnp.concatenate(tiles, axis=0)
    r_id = lax.broadcasted_iota(jnp.int32, (size, size), 0)
    c_id = lax.broadcasted_iota(jnp.int32, (size, size), 1)
    pivots = jnp.sum(jnp.where(r_id == c_id, whole, 0.0), axis=1, keepdims=True)
    root = jnp.sqrt(pivots)
    scaled = jnp.where(r_id == c_id, 1.0, whole) / root
    inverse = jnp.where(r_id >= c_id, scaled, 0.0)
    upper = jnp.where(r_id < c_id, scaled, jnp.where(r_id == c_id, root, 0.0))
    return upper.T, inverse


def factor_all(work, low, inv, between=None):
    n = work.shape[0]
    low[...] = jnp.zeros((n, n), jnp.float32)
    inv[...] = jnp.zeros((n, n), jnp.float32)

    def step(k, carry):
        at = pl.ds(pl.multiple_of(k * LANES, LANES), LANES)
        halfway = None if between is None else functools.partial(between, k, 0)
        block_low, block_inv = factor_block(work[at, at], halfway)
        rows = lax.broadcasted_iota(jnp.int32, (n, LANES), 0)
        panel = jnp.where(rows >= (k + 1) * LANES, dot(work[:, at], block_inv, 1, 1), 0.0)
        work[...] = work[...] - dot(panel, panel, 1, 1)
        left = dot(low[at, :], inv[...], 1, 0)
        low[:, at] = panel
        low[at, at] = block_low
        inv[at, :] = -dot(block_inv, left, 1, 0)
        inv[at, at] = block_inv
        if between is not None:
            between(k, 1)
        return carry

    lax.fori_loop(0, n // LANES, step, 0)


def exchange(sizes, cuts, win_units, diag_ref, panel, low, inv, held, window, pieces, work, sems):
    n_r, n_c, n_d = sizes
    total = n_r * n_c * n_d
    half = n_c // 2
    units = panel.shape[0]
    (diag_s, diag_r, ring_s, ring_r, deep_s, deep_r, w1_s, w1_r, w2_s, w2_r, w3_s, w3_r, own_s) = sems
    r, c, d = lax.axis_index("row"), lax.axis_index("col"), lax.axis_index("depth")
    position = (r * n_c + c) * n_d + d

    def remote(src, dst, send, recv, **where):
        return pltpu.make_async_remote_copy(
            src_ref=src,
            dst_ref=dst,
            send_sem=send,
            recv_sem=recv,
            device_id={"row": where.get("row", r), "col": where.get("col", c), "depth": where.get("depth", d)},
            device_id_type=pl.DeviceIdType.MESH,
        )

    def taker(block):
        return lax.div(block * n_d + d, n_c)

    def slot(block):
        return jnp.where(taker(block) == d, block * n_d + d - n_c * d, n_c + block)

    def at(h):
        return pl.ds(cuts[h], cuts[h + 1] - cuts[h])

    def send_diag(k, carry):
        to = lax.rem(position + k, total)
        remote(
            diag_ref, pieces.at[position], diag_s, diag_r,
            row=lax.div(to, n_c * n_d), col=lax.rem(lax.div(to, n_d), n_c), depth=lax.rem(to, n_d),
        ).start()
        return carry

    lax.fori_loop(1, total, send_diag, 0)
    pieces[position] = diag_ref[...]

    def window_parts():
        for p in range(-(-n_c * win_units // units)):
            for b in range(n_c):
                lo, hi = max(b * win_units, p * units), min((b + 1) * win_units, (p + 1) * units)
                if lo < hi:
                    yield p, b, lo, hi - lo

    def part(p, b, lo, count):
        src = panel.at[pl.ds(lo - p * units, count)]
        dst = window.at[pl.ds(lo - b * win_units, count)]
        if p == b * n_d:
            return pltpu.make_async_copy(src, dst, w1_r.at[p])
        return remote(src, dst, w1_s.at[p, b], w1_r.at[p], row=0, col=b, depth=0)

    root = jnp.logical_and(r == 0, d == 0)
    for p, b, lo, count in window_parts():
        @pl.when(position == p)
        def _(p=p, b=b, lo=lo, count=count):
            part(p, b, lo, count).start()

    def to_depth(k):
        return remote(window, window, w2_s.at[k], w2_r, depth=k)

    def to_row(k):
        return remote(window, window, w3_s.at[k], w3_r, row=k)

    def window_second():
        for p, b, lo, count in window_parts():
            @pl.when(jnp.logical_and(root, c == b))
            def _(p=p, b=b, lo=lo, count=count):
                if p == b * n_d:
                    part(p, b, lo, count).wait()
                else:
                    piece = window.at[pl.ds(lo - b * win_units, count)]
                    pltpu.make_async_copy(piece, piece, w1_r.at[p]).wait()

        @pl.when(root)
        def _():
            for k in range(1, n_d):
                to_depth(k).start()

    def window_third():
        @pl.when(jnp.logical_and(r == 0, d != 0))
        def _():
            pltpu.make_async_copy(window, window, w2_r).wait()

        @pl.when(r == 0)
        def _():
            for k in range(1, n_r):
                to_row(k).start()

    def ring(way, s, h):
        block = lax.rem(c + n_c - s + 1, n_c) if way == 0 else lax.rem(c + s - 1, n_c)
        to = lax.rem(c + 1, n_c) if way == 0 else lax.rem(c + n_c - 1, n_c)
        dst = held.at[slot(block), at(h)]
        src = panel.at[at(h)] if s == 1 else dst
        return remote(src, dst, ring_s.at[way, s - 1, h], ring_r.at[way, s - 1, h], col=to)

    def ring_parts(s):
        return [(0, 0), (1, 1)] + ([(0, 1), (1, 0)] if s < half else [])

    def deep(step, h):
        block = lax.rem(c + n_c - step, n_c)
        to = taker(block)
        index = block * n_d + d - n_c * to
        src = panel.at[at(h)] if step == 0 else held.at[slot(block), at(h)]
        where = step + half - 1
        return to, remote(
            src, held.at[index, at(h)], deep_s.at[where, h], deep_r.at[index, h], depth=to
        )

    def start_deep(step, h):
        to, copy = deep(step, h)

        @pl.when(to != d)
        def _():
            copy.start()

    def own_copy():
        return pltpu.make_async_copy(panel, held.at[slot(c)], own_s)

    for way, h in ring_parts(1):
        ring(way, 1, h).start()
    for h in range(2):
        start_deep(0, h)

    @pl.when(taker(c) == d)
    def _():
        own_copy().start()

    def arrived(s, parts):
        for way, h in parts:
            ring(way, s, h).wait_recv()
            if s < half and (s + 1 < half or way == h):
                ring(way, s + 1, h).start()
            step = s if (way == 0 or s == half) else -s
            start_deep(step, h)

    def between(k, later):
        def when(point, action):
            if point % 2 == later:
                pl.when(k == point // 2)(action)

        when(1, window_second)
        when(3, window_third)
        if half > 1:
            when(2, lambda: arrived(1, ring_parts(1)[:2]))
            when(6, lambda: arrived(1, ring_parts(1)[2:]))

    every = pieces.at[pl.ds(0, total - 1)]
    pltpu.make_async_copy(every, every, diag_r).wait()
    mine = diag_ref.shape[0]
    for p in range(total):
        work[p * mine : (p + 1) * mine, :] = pieces[p]
    factor_all(work, low, inv, between)

    for s in range(2 if half > 1 else 1, half + 1):
        arrived(s, ring_parts(s))

    @pl.when(r != 0)
    def _():
        pltpu.make_async_copy(window, window, w3_r).wait()

    for j in range(n_c):
        q = n_c * d + j

        @pl.when(lax.rem(q, n_d) != d)
        def _(j=j):
            for h in range(2):
                landed = held.at[j, at(h)]
                pltpu.make_async_copy(landed, landed, deep_r.at[j, h]).wait()

    pltpu.make_async_copy(every, every, diag_s).wait()
    for s in range(1, half + 1):
        for way, h in ring_parts(s):
            ring(way, s, h).wait_send()
    for step in range(1 - half, half + 1):
        for h in range(2):
            to, copy = deep(step, h)

            @pl.when(to != d)
            def _(copy=copy):
                copy.wait_send()

    @pl.when(taker(c) == d)
    def _():
        own_copy().wait()

    for p, b, lo, count in window_parts():
        if p != b * n_d:
            @pl.when(position == p)
            def _(p=p, b=b, lo=lo, count=count):
                part(p, b, lo, count).wait_send()

    @pl.when(root)
    def _():
        for k in range(1, n_d):
            to_depth(k).wait_send()

    @pl.when(r == 0)
    def _():
        for k in range(1, n_r):
            to_row(k).wait_send()


def exchange_call(sizes, diag_block, panel, win_units):
    n_r, n_c, n_d = sizes
    total = n_r * n_c * n_d
    units, unit, width = panel.shape
    n = diag_block.shape[1]
    square = jax.ShapeDtypeStruct((n, n), jnp.float32)
    vmem, anywhere = pl.BlockSpec(memory_space=pltpu.VMEM), pl.BlockSpec(memory_space=pl.ANY)
    dma, owners = pltpu.SemaphoreType.DMA, -(-n_c * win_units // units)
    sems = [
        dma, dma, dma((2, n_c // 2, 2)), dma((2, n_c // 2, 2)), dma((n_c, 2)), dma((n_c, 2)),
        dma((owners, n_c)), dma((owners,)), dma((n_d,)), dma, dma((n_r,)), dma, dma,
    ]
    return pl.pallas_call(
        functools.partial(exchange, sizes, (0, units // 2, units), win_units),
        out_shape=(
            square,
            square,
            jax.ShapeDtypeStruct((2 * n_c, units, unit, width), jnp.float32),
            jax.ShapeDtypeStruct((win_units, unit, width), jnp.float32),
        ),
        in_specs=[vmem, vmem],
        out_specs=(vmem, vmem, anywhere, anywhere),
        scratch_shapes=[
            pltpu.VMEM((total, diag_block.shape[0], n), jnp.float32),
            pltpu.VMEM((n, n), jnp.float32),
            sems,
        ],
        compiler_params=pltpu.CompilerParams(has_side_effects=True),
    )(diag_block, panel)


def body(sizes, diag_block, panel_rows, trailing):
    n_r, n_c, n_d = sizes
    position = (lax.axis_index("row") * n_c + lax.axis_index("col")) * n_d + lax.axis_index("depth")
    mine = diag_block.shape[0]
    own_rows, win_rows = trailing.shape
    rows, width = panel_rows.shape
    unit = math.gcd(rows, win_rows)
    low, inv, held, window = exchange_call(
        sizes, diag_block, panel_rows.reshape(rows // unit, unit, width), win_rows // unit
    )
    owned = held[:n_c].reshape(own_rows, width)
    own_factor = lax.dynamic_slice_in_dim(low, position * mine, mine, 0)
    solved = dot(panel_rows, inv, 1, 1)
    weight = dot(dot(window.reshape(win_rows, width), inv, 1, 1), inv, 1, 0)
    updated = trailing - dot(owned, weight, 1, 1)
    return (own_factor, solved, updated)


def solution(mesh):
    sizes = tuple(mesh.shape[axis] for axis in AXES)
    specs = (P(AXES, None), P(AXES, None), P(("row", "depth"), "col"))
    return jax.shard_map(
        functools.partial(body, sizes), mesh=mesh, in_specs=specs, out_specs=specs, check_vma=False
    )
```

```python
import functools
import math

import jax
import jax.numpy as jnp
from jax import lax
from jax.experimental import pallas as pl
from jax.experimental.pallas import tpu as pltpu
from jax.sharding import PartitionSpec as P

highest = lax.Precision.HIGHEST
AXES = ("row", "col", "depth")
LANES = 128


def dot(left, right, left_dim, right_dim):
    return lax.dot_general(
        left, right, (((left_dim,), (right_dim,)), ((), ())), precision=highest, preferred_element_type=jnp.float32
    )


def factor_block(block, halfway=None):
    size = block.shape[0]
    lane = lax.broadcasted_iota(jnp.int32, (8, size), 1)
    sub = lax.broadcasted_iota(jnp.int32, (8, size), 0)
    tiles = [block[8 * i : 8 * i + 8, :] for i in range(size // 8)]
    for j in range(size):
        if halfway is not None and j == size // 2:
            halfway()
        t, s = divmod(j, 8)
        row = tiles[t][s : s + 1, :]
        inverse = 1.0 / row[:, j : j + 1]
        source = jnp.where(lane[0:1] == j, 1.0, row) * inverse
        for i in range(t, size // 8):
            if i == t and s == 7:
                continue
            tile = tiles[i]
            new = jnp.where(lane == j, 0.0, tile) - tile[:, j : j + 1] * source
            tiles[i] = jnp.where(sub > s, new, tile) if i == t else new
    whole = jnp.concatenate(tiles, axis=0)
    r_id = lax.broadcasted_iota(jnp.int32, (size, size), 0)
    c_id = lax.broadcasted_iota(jnp.int32, (size, size), 1)
    pivots = jnp.sum(jnp.where(r_id == c_id, whole, 0.0), axis=1, keepdims=True)
    root = jnp.sqrt(pivots)
    scaled = jnp.where(r_id == c_id, 1.0, whole) / root
    inverse = jnp.where(r_id >= c_id, scaled, 0.0)
    upper = jnp.where(r_id < c_id, scaled, jnp.where(r_id == c_id, root, 0.0))
    return upper.T, inverse


def factor_all(work, low, inv, between=None):
    n = work.shape[0]
    low[...] = jnp.zeros((n, n), jnp.float32)
    inv[...] = jnp.zeros((n, n), jnp.float32)

    def step(k, carry):
        at = pl.ds(pl.multiple_of(k * LANES, LANES), LANES)
        halfway = None if between is None else functools.partial(between, k, 0)
        block_low, block_inv = factor_block(work[at, at], halfway)
        rows = lax.broadcasted_iota(jnp.int32, (n, LANES), 0)
        panel = jnp.where(rows >= (k + 1) * LANES, dot(work[:, at], block_inv, 1, 1), 0.0)
        work[...] = work[...] - dot(panel, panel, 1, 1)
        left = dot(low[at, :], inv[...], 1, 0)
        low[:, at] = panel
        low[at, at] = block_low
        inv[at, :] = -dot(block_inv, left, 1, 0)
        inv[at, at] = block_inv
        if between is not None:
            between(k, 1)
        return carry

    lax.fori_loop(0, n // LANES, step, 0)


def exchange(sizes, cuts, win_units, diag_ref, panel, low, weight, solved, held, window, pieces, work, inv, sems):
    n_r, n_c, n_d = sizes
    total = n_r * n_c * n_d
    half = n_c // 2
    units = panel.shape[0]
    (diag_s, diag_r, ring_s, ring_r, deep_s, deep_r, w1_s, w1_r, w2_s, w2_r, w3_s, w3_r, own_s) = sems
    r, c, d = lax.axis_index("row"), lax.axis_index("col"), lax.axis_index("depth")
    position = (r * n_c + c) * n_d + d

    def remote(src, dst, send, recv, **where):
        return pltpu.make_async_remote_copy(
            src_ref=src,
            dst_ref=dst,
            send_sem=send,
            recv_sem=recv,
            device_id={"row": where.get("row", r), "col": where.get("col", c), "depth": where.get("depth", d)},
            device_id_type=pl.DeviceIdType.MESH,
        )

    def taker(block):
        return lax.div(block * n_d + d, n_c)

    def slot(block):
        return jnp.where(taker(block) == d, block * n_d + d - n_c * d, n_c + block)

    def at(h):
        return pl.ds(cuts[h], cuts[h + 1] - cuts[h])

    def send_diag(k, carry):
        to = lax.rem(position + k, total)
        remote(
            diag_ref, pieces.at[position], diag_s, diag_r,
            row=lax.div(to, n_c * n_d), col=lax.rem(lax.div(to, n_d), n_c), depth=lax.rem(to, n_d),
        ).start()
        return carry

    lax.fori_loop(1, total, send_diag, 0)
    pieces[position] = diag_ref[...]

    def window_parts():
        for p in range(-(-n_c * win_units // units)):
            for b in range(n_c):
                lo, hi = max(b * win_units, p * units), min((b + 1) * win_units, (p + 1) * units)
                if lo < hi:
                    yield p, b, lo, hi - lo

    def part(p, b, lo, count):
        src = panel.at[pl.ds(lo - p * units, count)]
        dst = window.at[pl.ds(lo - b * win_units, count)]
        if p == b * n_d:
            return pltpu.make_async_copy(src, dst, w1_r.at[p])
        return remote(src, dst, w1_s.at[p, b], w1_r.at[p], row=0, col=b, depth=0)

    root = jnp.logical_and(r == 0, d == 0)
    for p, b, lo, count in window_parts():
        @pl.when(position == p)
        def _(p=p, b=b, lo=lo, count=count):
            part(p, b, lo, count).start()

    def to_depth(k):
        return remote(window, window, w2_s.at[k], w2_r, depth=k)

    def to_row(k):
        return remote(window, window, w3_s.at[k], w3_r, row=k)

    def window_second():
        for p, b, lo, count in window_parts():
            @pl.when(jnp.logical_and(root, c == b))
            def _(p=p, b=b, lo=lo, count=count):
                if p == b * n_d:
                    part(p, b, lo, count).wait()
                else:
                    piece = window.at[pl.ds(lo - b * win_units, count)]
                    pltpu.make_async_copy(piece, piece, w1_r.at[p]).wait()

        @pl.when(root)
        def _():
            for k in range(1, n_d):
                to_depth(k).start()

    def window_third():
        @pl.when(jnp.logical_and(r == 0, d != 0))
        def _():
            pltpu.make_async_copy(window, window, w2_r).wait()

        @pl.when(r == 0)
        def _():
            for k in range(1, n_r):
                to_row(k).start()

    def ring(way, s, h):
        block = lax.rem(c + n_c - s + 1, n_c) if way == 0 else lax.rem(c + s - 1, n_c)
        to = lax.rem(c + 1, n_c) if way == 0 else lax.rem(c + n_c - 1, n_c)
        dst = held.at[slot(block), at(h)]
        src = panel.at[at(h)] if s == 1 else dst
        return remote(src, dst, ring_s.at[way, s - 1, h], ring_r.at[way, s - 1, h], col=to)

    def ring_parts(s):
        return [(0, 0), (1, 1)] + ([(0, 1), (1, 0)] if s < half else [])

    def deep(step, h):
        block = lax.rem(c + n_c - step, n_c)
        to = taker(block)
        index = block * n_d + d - n_c * to
        src = panel.at[at(h)] if step == 0 else held.at[slot(block), at(h)]
        where = step + half - 1
        return to, remote(
            src, held.at[index, at(h)], deep_s.at[where, h], deep_r.at[index, h], depth=to
        )

    def start_deep(step, h):
        to, copy = deep(step, h)

        @pl.when(to != d)
        def _():
            copy.start()

    def own_copy():
        return pltpu.make_async_copy(panel, held.at[slot(c)], own_s)

    for way, h in ring_parts(1):
        ring(way, 1, h).start()
    for h in range(2):
        start_deep(0, h)

    @pl.when(taker(c) == d)
    def _():
        own_copy().start()

    def arrived(s, parts):
        for way, h in parts:
            ring(way, s, h).wait_recv()
            if s < half and (s + 1 < half or way == h):
                ring(way, s + 1, h).start()
            step = s if (way == 0 or s == half) else -s
            start_deep(step, h)

    def between(k, later):
        def when(point, action):
            if point % 2 == later:
                pl.when(k == point // 2)(action)

        when(1, window_second)
        when(3, window_third)
        if half > 1:
            when(2, lambda: arrived(1, ring_parts(1)[:2]))
            when(6, lambda: arrived(1, ring_parts(1)[2:]))

    every = pieces.at[pl.ds(0, total - 1)]
    pltpu.make_async_copy(every, every, diag_r).wait()
    mine = diag_ref.shape[0]
    for p in range(total):
        work[p * mine : (p + 1) * mine, :] = pieces[p]
    factor_all(work, low, inv, between)

    @pl.when(r != 0)
    def _():
        pltpu.make_async_copy(window, window, w3_r).wait()

    weight[...] = dot(dot(window[...].reshape(weight.shape), inv[...], 1, 1), inv[...], 1, 0)
    solved[...] = dot(panel[...].reshape(solved.shape), inv[...], 1, 1)
    for s in range(2 if half > 1 else 1, half + 1):
        arrived(s, ring_parts(s))

    for j in range(n_c):
        q = n_c * d + j

        @pl.when(lax.rem(q, n_d) != d)
        def _(j=j):
            for h in range(2):
                landed = held.at[j, at(h)]
                pltpu.make_async_copy(landed, landed, deep_r.at[j, h]).wait()

    pltpu.make_async_copy(every, every, diag_s).wait()
    for s in range(1, half + 1):
        for way, h in ring_parts(s):
            ring(way, s, h).wait_send()
    for step in range(1 - half, half + 1):
        for h in range(2):
            to, copy = deep(step, h)

            @pl.when(to != d)
            def _(copy=copy):
                copy.wait_send()

    @pl.when(taker(c) == d)
    def _():
        own_copy().wait()

    for p, b, lo, count in window_parts():
        if p != b * n_d:
            @pl.when(position == p)
            def _(p=p, b=b, lo=lo, count=count):
                part(p, b, lo, count).wait_send()

    @pl.when(root)
    def _():
        for k in range(1, n_d):
            to_depth(k).wait_send()

    @pl.when(r == 0)
    def _():
        for k in range(1, n_r):
            to_row(k).wait_send()


def exchange_call(sizes, diag_block, panel, win_units):
    n_r, n_c, n_d = sizes
    total = n_r * n_c * n_d
    units, unit, width = panel.shape
    n = diag_block.shape[1]
    square = jax.ShapeDtypeStruct((n, n), jnp.float32)
    vmem, anywhere = pl.BlockSpec(memory_space=pltpu.VMEM), pl.BlockSpec(memory_space=pl.ANY)
    dma, owners = pltpu.SemaphoreType.DMA, -(-n_c * win_units // units)
    sems = [
        dma, dma, dma((2, n_c // 2, 2)), dma((2, n_c // 2, 2)), dma((n_c, 2)), dma((n_c, 2)),
        dma((owners, n_c)), dma((owners,)), dma((n_d,)), dma, dma((n_r,)), dma, dma,
    ]
    return pl.pallas_call(
        functools.partial(exchange, sizes, (0, units // 2, units), win_units),
        out_shape=(
            square,
            jax.ShapeDtypeStruct((win_units * unit, width), jnp.float32),
            jax.ShapeDtypeStruct((units * unit, width), jnp.float32),
            jax.ShapeDtypeStruct((2 * n_c, units, unit, width), jnp.float32),
        ),
        in_specs=[vmem, vmem],
        out_specs=(vmem, vmem, vmem, anywhere),
        scratch_shapes=[
            pltpu.VMEM((win_units, unit, width), jnp.float32),
            pltpu.VMEM((total, diag_block.shape[0], n), jnp.float32),
            pltpu.VMEM((n, n), jnp.float32),
            pltpu.VMEM((n, n), jnp.float32),
            sems,
        ],
        compiler_params=pltpu.CompilerParams(has_side_effects=True),
    )(diag_block, panel)


def update(held, weight, trailing, out):
    out[...] = trailing[...] - dot(held[...], weight[...], 1, 1)


def update_call(held, weight, trailing):
    rows, columns = trailing.shape
    width = held.shape[1]
    chunk = max(m for m in range(8, 1025, 8) if rows % m == 0)
    return pl.pallas_call(
        update,
        grid=(rows // chunk,),
        out_shape=jax.ShapeDtypeStruct(trailing.shape, jnp.float32),
        in_specs=[
            pl.BlockSpec((chunk, width), lambda i: (i, 0)),
            pl.BlockSpec((columns, width), lambda i: (0, 0)),
            pl.BlockSpec((chunk, columns), lambda i: (i, 0)),
        ],
        out_specs=pl.BlockSpec((chunk, columns), lambda i: (i, 0)),
    )(held, weight, trailing)


def body(sizes, diag_block, panel_rows, trailing):
    n_r, n_c, n_d = sizes
    position = (lax.axis_index("row") * n_c + lax.axis_index("col")) * n_d + lax.axis_index("depth")
    mine = diag_block.shape[0]
    own_rows, win_rows = trailing.shape
    rows, width = panel_rows.shape
    unit = math.gcd(rows, win_rows)
    low, weight, solved, held = exchange_call(
        sizes, diag_block, panel_rows.reshape(rows // unit, unit, width), win_rows // unit
    )
    own_factor = lax.dynamic_slice_in_dim(low, position * mine, mine, 0)
    updated = update_call(held.reshape(2 * n_c * rows, width), weight, trailing)
    return (own_factor, solved, updated)


def solution(mesh):
    sizes = tuple(mesh.shape[axis] for axis in AXES)
    specs = (P(AXES, None), P(AXES, None), P(("row", "depth"), "col"))
    return jax.shard_map(
        functools.partial(body, sizes), mesh=mesh, in_specs=specs, out_specs=specs, check_vma=False
    )
```
